32 devices in a mesh: row: 4 (over z), col: 8 (over y, x, core).
Axes of the slice: x: 2, y: 2, z: 4, core: 2. Of those that a mesh axis runs over, the one named last changes fastest.
Arguments:
- grad: float32 [8192, 14336], P(('row', 'col')), may hold values from -30 to 30
- momentum: float32 [8192, 14336], P(('row', 'col')), may hold values from -6 to 6
- weight: float32 [8192, 14336], P(('row', 'col')), may hold values from -0.75 to 0.75
Outputs:
- new_weight: float32 [8192, 14336], P('row', 'col')
- new_momentum: float32 [8192, 14336], P('row', 'col')
The draws below stay inside these ranges and needn't reach their ends.
All inputs are finite; a program needn't handle non-finite values.
Results may differ from the reference program's by a relative error of at most 0.00002.
Values sent between devices are 32-bit elements; how exact they have to be, the bound alone decides.
No kernel may reach another device: no remote copies, remote signals or barrier semaphores. Data moves between devices by JAX's collectives and lax.ppermute only.
A program may use at most 192 MiB of HBM per device.

```python
import math
import jax
import jax.numpy as jnp

D = 8192
FF = 14336


def draw_grad(key, part):
    key_rows, key_cols, key_base = jax.random.split(key, 3)
    row_scale = jnp.exp(jax.random.uniform(key_rows, (D, 1), jnp.float32) * jnp.log(10.0))
    col_scale = jnp.exp(jax.random.uniform(key_cols, (1, FF), jnp.float32) * jnp.log(10.0))
    ramp = 1.0 + 2.0 * jnp.arange(D, dtype=jnp.float32).reshape(D, 1) / (D - 1)
    base = jnp.clip(jax.random.normal(key_base, (D, FF), jnp.float32), -6.0, 6.0)
    scaled = base * row_scale * col_scale * ramp / 10.0
    return jnp.clip(scaled, -30.0, 30.0).astype(jnp.float32)


def levels(stream_key, extent, shards, low, high):
    level, own = 1.0, jax.random.fold_in(stream_key, 6)
    for position, shards_of in shards:
        draws = jnp.exp(jax.random.uniform(jax.random.fold_in(own, position), (shards_of,), jnp.float32, low / len(shards), high / len(shards)))
        level = level * jnp.repeat(draws, extent[position] // shards_of).reshape([-1 if axis == position else 1 for axis in range(len(extent))])
    return level


def gaussian(rng, shape, deviation, bound, shards=(), held_as=jnp.bfloat16):
    loudness = levels(rng, shape, shards, -0.22, 0.18) if shards else 1.0
    drawn = jax.random.normal(rng, shape, jnp.float32) * deviation * loudness
    return jnp.minimum(jnp.maximum(drawn, -bound), bound).astype(held_as)


def setup_inputs(seed: int = 0) -> dict:
    seeds = jax.random.split(jax.random.key(seed), 4)
    return {
        "grad": draw_grad(jax.random.fold_in(seeds[3], 71), 0),
        "momentum": gaussian(seeds[1], (D, FF), 1.0, 6.0, ((0, 32),), jnp.float32),
        "weight": gaussian(seeds[2], (D, FF), 0.05, 0.75, ((0, 32),), jnp.float32),
    }


def reference(grad, momentum, weight):
    total = jnp.sum(grad * grad)
    limit = jnp.float32(math.sqrt(D * FF))
    factor = jnp.minimum(jnp.float32(1.0), limit / (jnp.sqrt(total) + jnp.float32(1e-06)))
    new_momentum = jnp.float32(0.9) * momentum + factor * grad
    new_weight = weight - jnp.float32(0.1) * new_momentum
    return (new_weight, new_momentum)
```

```python
import math

import jax
import jax.numpy as jnp
from jax import lax
from jax.experimental import pallas as pl
from jax.experimental.pallas import tpu as pltpu
from jax.sharding import PartitionSpec as P


F32 = jnp.float32
LANES = 128


def hop(x, axis, k, n):
    return lax.ppermute(x, axis, [(i, i ^ k) for i in range(n)])


def cost(passes, rows, cols):
    return pl.CostEstimate(flops=4 * rows * cols, bytes_accessed=4 * passes * rows * cols, transcendentals=0)


PARAMS = pltpu.CompilerParams(vmem_limit_bytes=67043328)


def block_rows(rows, start, most=64):
    b = most
    while rows % b or start % b:
        b //= 2
    return b


def copy_kernel(at, x_ref, o_ref):
    o_ref[...] = x_ref[...]


def cut(x, at, cols, start, rows):
    b = block_rows(rows, start)
    s = start // b
    return pl.pallas_call(
        copy_kernel,
        grid_spec=pltpu.PrefetchScalarGridSpec(
            num_scalar_prefetch=1, grid=(rows // b,),
            in_specs=[pl.BlockSpec((b, cols), lambda i, at: (s + i, at[0]))],
            out_specs=pl.BlockSpec((b, cols), lambda i, at: (i, 0))),
        out_shape=jax.ShapeDtypeStruct((rows, cols), F32),
        cost_estimate=cost(2, rows, cols), name="cut", compiler_params=PARAMS,
    )(at, x)


def calc_kernel(at, factor, m_ref, g_ref, o_ref):
    o_ref[...] = F32(0.9) * m_ref[...] + factor[0] * g_ref[...]


def calc(m, g, factor, at, cols, start, rows):
    b = block_rows(rows, start)
    s = start // b
    spec = pl.BlockSpec((b, cols), lambda i, at: (s + i, at[0]))
    return pl.pallas_call(
        calc_kernel,
        grid_spec=pltpu.PrefetchScalarGridSpec(
            num_scalar_prefetch=1, grid=(rows // b,),
            in_specs=[pl.BlockSpec(memory_space=pltpu.SMEM), spec, spec],
            out_specs=pl.BlockSpec((b, cols), lambda i, at: (i, 0))),
        out_shape=jax.ShapeDtypeStruct((rows, cols), F32),
        cost_estimate=cost(3, rows, cols), name="calc", compiler_params=PARAMS,
    )(at, factor, m, g)


def finish_kernel(at, w_ref, m_ref, *refs):
    nw_ref, nm_ref = refs[-2:]
    m = m_ref[...]
    nm_ref[...] = m
    nw_ref[...] = w_ref[...] - F32(0.1) * m


def finish(at, w, m, outs, shape, piece, start):
    rows, cols = w.shape
    b = block_rows(rows, start)
    s, p = start // b, piece // b
    spec = pl.BlockSpec((b, cols), lambda i, at: (i, 0))
    ospec = pl.BlockSpec((b, cols), lambda i, at: (at[0] * p + s + i, 0))
    hbm = pl.BlockSpec(memory_space=pl.ANY)
    outs = outs or ()
    return pl.pallas_call(
        finish_kernel,
        grid_spec=pltpu.PrefetchScalarGridSpec(
            num_scalar_prefetch=1, grid=(rows // b,),
            in_specs=[spec, spec] + [hbm] * len(outs), out_specs=[ospec, ospec]),
        out_shape=[jax.ShapeDtypeStruct(shape, F32)] * 2,
        input_output_aliases={3: 0, 4: 1} if outs else {},
        cost_estimate=cost(4, rows, cols), name="finish", compiler_params=PARAMS,
    )(at, w, m, *outs)


def own_kernel(at, factor, w_ref, m_ref, g_ref, nw_ref, nm_ref):
    m = F32(0.9) * m_ref[...] + factor[0] * g_ref[...]
    nm_ref[...] = m
    nw_ref[...] = w_ref[...] - F32(0.1) * m


def own(at, factor, w, m, g, n):
    rows, cols = w.shape[0], w.shape[1] // n
    b = block_rows(rows, 0)
    t = rows // b
    spec = pl.BlockSpec((b, cols), lambda i, at: (i, at[0]))
    ospec = pl.BlockSpec((b, cols), lambda i, at: (at[0] * t + i, 0))
    return pl.pallas_call(
        own_kernel,
        grid_spec=pltpu.PrefetchScalarGridSpec(
            num_scalar_prefetch=1, grid=(t,),
            in_specs=[pl.BlockSpec(memory_space=pltpu.SMEM)] + [spec] * 3, out_specs=[ospec, ospec]),
        out_shape=[jax.ShapeDtypeStruct((rows * n, cols), F32)] * 2,
        cost_estimate=cost(5, rows, cols), name="own", compiler_params=PARAMS,
    )(at, factor, w, m, g)


def squares_kernel(g_ref, o_ref, acc_ref):
    i = pl.program_id(0)
    rows, ff = g_ref.shape

    @pl.when(i == 0)
    def _():
        acc_ref[...] = jnp.zeros_like(acc_ref)

    for c in range(0, ff, LANES):
        g = g_ref[:, c:c + LANES]
        acc_ref[:, c:c + LANES] += jnp.sum((g * g).reshape(rows // 8, 8, LANES), axis=0)

    @pl.when(i == pl.num_programs(0) - 1)
    def _():
        parts = [acc_ref[:, c:c + LANES] for c in range(0, ff, LANES)]
        while len(parts) > 1:
            parts = [sum(parts[j:j + 2]) for j in range(0, len(parts), 2)]
        o_ref[...] = parts[0]


def squares(g):
    rows, ff = g.shape
    b = block_rows(rows, 0, 32)
    return pl.pallas_call(
        squares_kernel,
        grid=(rows // b,),
        in_specs=[pl.BlockSpec((b, ff), lambda i: (i, 0))],
        out_specs=pl.BlockSpec((8, LANES), lambda i: (0, 0)),
        out_shape=jax.ShapeDtypeStruct((8, LANES), F32),
        scratch_shapes=[pltpu.VMEM((8, ff), F32)],
        cost_estimate=cost(1, rows, ff), name="squares", compiler_params=PARAMS,
    )(g)


def parcels(k, n, rows):
    e = rows // 8
    if e % 8 == 0 and k == n - 1:
        return [(0, e), (e, 3 * e), (4 * e, 4 * e)]
    return [(0, rows)]


def plan(n):
    far = list(range(n - 1, 3, -1))
    near = [k for k in (3, 2, 1) if k < n]
    return far, near


def body(limit, n, nrow, grad, momentum, weight):
    me = lax.axis_index("col")
    rows, ff = weight.shape
    cols = ff // n
    far, near = plan(n)
    at = {k: jnp.reshape(me ^ k, (1,)).astype(jnp.int32) for k in range(n)}
    moved_w, moved_m = {}, {}

    def send_w(k):
        for j, (s, r) in enumerate(parcels(k, n, rows)):
            moved_w[k, j] = hop(cut(weight, at[k], cols, s, r), "col", k, n)

    for k in far + near:
        send_w(k)
    part = squares(grad)
    bits = rounds(n, nrow)
    for axis, k, size in bits:
        part = part + hop(part, axis, k, size)
    total = jnp.sum(part)
    factor = jnp.reshape(jnp.minimum(F32(1.0), limit / (jnp.sqrt(total) + F32(1e-06))), (1,))
    for k in far + near:
        for j, (s, r) in enumerate(parcels(k, n, rows)):
            moved_m[k, j] = hop(calc(momentum, grad, factor, at[k], cols, s, r), "col", k, n)
    outs = own(at[0], factor, weight, momentum, grad, n)
    for k in finish_order(n):
        for j, (s, r) in enumerate(parcels(k, n, rows)):
            outs = finish(at[k], moved_w[k, j], moved_m[k, j], outs, (rows * n, cols), rows, s)
    return tuple(outs)


def finish_order(n):
    first = [k for k in (1, 7, 6, 5, 3, 4, 2) if k < n]
    return list(range(n - 1, 7, -1)) + first


def rounds(n, nrow):
    col = [("col", 1 << j, n) for j in range(n.bit_length() - 1)]
    row = [("row", 1 << j, nrow) for j in range(nrow.bit_length() - 1)]
    return col[2:] + col[:1] + row + col[1:2]


def solution(mesh):
    spec = P(("row", "col"), None)
    n, nrow = mesh.shape["col"], mesh.shape["row"]

    def run(grad, momentum, weight):
        limit = F32(math.sqrt(grad.shape[0] * grad.shape[1]))
        f = jax.shard_map(lambda g, m, w: body(limit, n, nrow, g, m, w), mesh=mesh, in_specs=(spec,) * 3, out_specs=(P("row", "col"),) * 2, check_vma=False)
        return f(grad, momentum, weight)

    return run
```

```python
import functools
import math

import jax
import jax.numpy as jnp
from jax import lax
from jax.experimental import pallas as pl
from jax.experimental.pallas import tpu as pltpu
from jax.sharding import PartitionSpec as P


F32 = jnp.float32
LANES = 128


def hop(x, axis, k, n):
    return lax.ppermute(x, axis, [(i, i ^ k) for i in range(n)])


def cost(passes, rows, cols):
    return pl.CostEstimate(flops=4 * rows * cols, bytes_accessed=4 * passes * rows * cols, transcendentals=0)


PARAMS = pltpu.CompilerParams(vmem_limit_bytes=67043328)


def block_rows(rows, start, most=256):
    b = most
    while rows % b or start % b:
        b //= 2
    return b


def copy_kernel(at, x_ref, o_ref):
    o_ref[...] = x_ref[...]


def cut(x, at, cols, start, rows):
    b = block_rows(rows, start)
    s = start // b
    return pl.pallas_call(
        copy_kernel,
        grid_spec=pltpu.PrefetchScalarGridSpec(
            num_scalar_prefetch=1, grid=(rows // b,),
            in_specs=[pl.BlockSpec((b, cols), lambda i, at: (s + i, at[0]))],
            out_specs=pl.BlockSpec((b, cols), lambda i, at: (i, 0))),
        out_shape=jax.ShapeDtypeStruct((rows, cols), F32),
        cost_estimate=cost(2, rows, cols), name="cut", compiler_params=PARAMS,
    )(at, x)


def calc_kernel(at, factor, m_ref, g_ref, o_ref):
    o_ref[...] = F32(0.9) * m_ref[...] + factor[0] * g_ref[...]


def calc(m, g, factor, at, cols, start, rows):
    b = block_rows(rows, start)
    s = start // b
    spec = pl.BlockSpec((b, cols), lambda i, at: (s + i, at[0]))
    return pl.pallas_call(
        calc_kernel,
        grid_spec=pltpu.PrefetchScalarGridSpec(
            num_scalar_prefetch=1, grid=(rows // b,),
            in_specs=[pl.BlockSpec(memory_space=pltpu.SMEM), spec, spec],
            out_specs=pl.BlockSpec((b, cols), lambda i, at: (i, 0))),
        out_shape=jax.ShapeDtypeStruct((rows, cols), F32),
        cost_estimate=cost(3, rows, cols), name="calc", compiler_params=PARAMS,
    )(at, factor, m, g)


def finish_kernel(parts, at, *refs):
    nw_ref, nm_ref = refs[-2:]
    for q in range(parts):
        @pl.when(pl.program_id(0) == q)
        def _():
            m = refs[2 * q + 1][...]
            nm_ref[...] = m
            nw_ref[...] = refs[2 * q][...] - F32(0.1) * m


def finish(at, pairs, outs, shape, piece, start, rows, within):
    cols = shape[1]
    b = block_rows(rows, start)
    s, p, o = start // b, piece // b, within // b
    parts = len(pairs)
    last = rows // b - 1

    def spec(part, first):
        def index(q, i, at):
            turn = jnp.where(q == part, i, jnp.where(q < part, 0, last))
            return (first + turn, 0)

        return pl.BlockSpec((b, cols), index if parts > 1 else lambda q, i, at: (first + i, 0))

    ospec = pl.BlockSpec((b, cols), lambda q, i, at: (at[q] * p + s + i, 0))
    hbm = pl.BlockSpec(memory_space=pl.ANY)
    return pl.pallas_call(
        functools.partial(finish_kernel, parts),
        grid_spec=pltpu.PrefetchScalarGridSpec(
            num_scalar_prefetch=1, grid=(parts, rows // b),
            in_specs=[spec(part, first) for part in range(parts) for first in (o, 0)] + [hbm] * 2, out_specs=[ospec, ospec]),
        out_shape=[jax.ShapeDtypeStruct(shape, F32)] * 2,
        input_output_aliases={2 * parts + 1: 0, 2 * parts + 2: 1},
        cost_estimate=cost(4 * parts, rows, cols), name="finish", compiler_params=PARAMS,
    )(at, *[x for pair in pairs for x in pair], *outs)


def own_kernel(at, factor, w_ref, m_ref, g_ref, nw_ref, nm_ref):
    m = F32(0.9) * m_ref[...] + factor[0] * g_ref[...]
    nm_ref[...] = m
    nw_ref[...] = w_ref[...] - F32(0.1) * m


def own(at, factor, w, m, g, n):
    rows, cols = w.shape[0], w.shape[1] // n
    b = block_rows(rows, 0)
    t = rows // b
    spec = pl.BlockSpec((b, cols), lambda i, at: (i, at[0]))
    ospec = pl.BlockSpec((b, cols), lambda i, at: (at[0] * t + i, 0))
    return pl.pallas_call(
        own_kernel,
        grid_spec=pltpu.PrefetchScalarGridSpec(
            num_scalar_prefetch=1, grid=(t,),
            in_specs=[pl.BlockSpec(memory_space=pltpu.SMEM)] + [spec] * 3, out_specs=[ospec, ospec]),
        out_shape=[jax.ShapeDtypeStruct((rows * n, cols), F32)] * 2,
        cost_estimate=cost(5, rows, cols), name="own", compiler_params=PARAMS,
    )(at, factor, w, m, g)


def squares_kernel(g_ref, o_ref, acc_ref):
    i = pl.program_id(0)
    rows, ff = g_ref.shape

    @pl.when(i == 0)
    def _():
        acc_ref[...] = jnp.zeros_like(acc_ref)

    for c in range(0, ff, LANES):
        g = g_ref[:, c:c + LANES]
        acc_ref[:, c:c + LANES] += jnp.sum((g * g).reshape(rows // 8, 8, LANES), axis=0)

    @pl.when(i == pl.num_programs(0) - 1)
    def _():
        parts = [acc_ref[:, c:c + LANES] for c in range(0, ff, LANES)]
        while len(parts) > 1:
            parts = [sum(parts[j:j + 2]) for j in range(0, len(parts), 2)]
        o_ref[...] = parts[0]


def squares(g):
    rows, ff = g.shape
    b = block_rows(rows, 0, 32)
    return pl.pallas_call(
        squares_kernel,
        grid=(rows // b,),
        in_specs=[pl.BlockSpec((b, ff), lambda i: (i, 0))],
        out_specs=pl.BlockSpec((8, LANES), lambda i: (0, 0)),
        out_shape=jax.ShapeDtypeStruct((8, LANES), F32),
        scratch_shapes=[pltpu.VMEM((8, ff), F32)],
        cost_estimate=cost(1, rows, ff), name="squares", compiler_params=PARAMS,
    )(g)


def last_pair(n):
    return [k for k in (4, 2) if k < n]


def w_parcels(k, n, rows):
    e = rows // 8
    if e % 8 == 0 and k == n - 1:
        return [(0, e), (e, 3 * e), (4 * e, 4 * e)]
    return [(0, rows)]


SPLIT = lambda e: [(0, 4 * e), (4 * e, 2 * e), (6 * e, e), (7 * e, e)]


def m_parcels(k, n, rows):
    e = rows // 8
    if e % 8 == 0 and k in last_pair(n):
        return SPLIT(e)
    return w_parcels(k, n, rows)


def plan(n):
    far = list(range(n - 1, 3, -1))
    near = [k for k in (3, 2, 1) if k < n]
    return far, near


def body(limit, n, nrow, grad, momentum, weight):
    me = lax.axis_index("col")
    rows, ff = weight.shape
    cols = ff // n
    far, near = plan(n)
    at = {k: jnp.reshape(me ^ k, (1,)).astype(jnp.int32) for k in range(n)}
    moved_w, moved_m = {}, {}

    def send_w(k):
        for j, (s, r) in enumerate(w_parcels(k, n, rows)):
            moved_w[k, j] = hop(cut(weight, at[k], cols, s, r), "col", k, n)

    for k in far + near:
        send_w(k)
    part = squares(grad)
    bits = rounds(n, nrow)
    for axis, k, size in bits:
        part = part + hop(part, axis, k, size)
    total = jnp.sum(part)
    factor = jnp.reshape(jnp.minimum(F32(1.0), limit / (jnp.sqrt(total) + F32(1e-06))), (1,))
    for k in far + near:
        for j, (s, r) in enumerate(m_parcels(k, n, rows)):
            moved_m[k, j] = hop(calc(momentum, grad, factor, at[k], cols, s, r), "col", k, n)
    outs = own(at[0], factor, weight, momentum, grad, n)
    for group in finish_order(n, rows):
        (s, r) = m_parcels(group[0][0], n, rows)[group[0][1]]
        pairs, where = [], []
        for k, j in group:
            i = max(i for i, (ws, _) in enumerate(w_parcels(k, n, rows)) if ws <= s)
            pairs.append((moved_w[k, i], moved_m[k, j]))
            where.append(at[k])
        within = s - w_parcels(group[0][0], n, rows)[i][0]
        outs = finish(jnp.concatenate(where), pairs, outs, (rows * n, cols), rows, s, r, within)
    return tuple(outs)


def finish_order(n, rows):
    end = last_pair(n)
    order = [1] + [k for k in range(n - 1, 1, -1) if k not in end]
    groups = [[(k, j)] for k in order for j in range(len(m_parcels(k, n, rows)))]
    for j in range(len(m_parcels(end[0], n, rows))):
        groups.append([(k, j) for k in end])
    return groups


def rounds(n, nrow):
    col = [("col", 1 << j, n) for j in range(n.bit_length() - 1)]
    row = [("row", 1 << j, nrow) for j in range(nrow.bit_length() - 1)]
    return col[2:] + col[:1] + row + col[1:2]


def solution(mesh):
    spec = P(("row", "col"), None)
    n, nrow = mesh.shape["col"], mesh.shape["row"]

    def run(grad, momentum, weight):
        limit = F32(math.sqrt(grad.shape[0] * grad.shape[1]))
        f = jax.shard_map(lambda g, m, w: body(limit, n, nrow, g, m, w), mesh=mesh, in_specs=(spec,) * 3, out_specs=(P("row", "col"),) * 2, check_vma=False)
        return f(grad, momentum, weight)

    return run
```

```python
import functools
import math

import jax
import jax.numpy as jnp
from jax import lax
from jax.experimental import pallas as pl
from jax.experimental.pallas import tpu as pltpu
from jax.sharding import PartitionSpec as P


F32 = jnp.float32
LANES = 128


def hop(x, axis, k, n):
    return lax.ppermute(x, axis, [(i, i ^ k) for i in range(n)])


def cost(passes, rows, cols):
    return pl.CostEstimate(flops=4 * rows * cols, bytes_accessed=4 * passes * rows * cols, transcendentals=0)


PARAMS = pltpu.CompilerParams(vmem_limit_bytes=67043328)


def block_rows(rows, start, most=256):
    b = most
    while rows % b or start % b:
        b //= 2
    return b


def copy_kernel(at, x_ref, o_ref):
    o_ref[...] = x_ref[...]


def cut(x, at, cols, start, rows):
    b = block_rows(rows, start)
    s = start // b
    return pl.pallas_call(
        copy_kernel,
        grid_spec=pltpu.PrefetchScalarGridSpec(
            num_scalar_prefetch=1, grid=(rows // b,),
            in_specs=[pl.BlockSpec((b, cols), lambda i, at: (s + i, at[0]))],
            out_specs=pl.BlockSpec((b, cols), lambda i, at: (i, 0))),
        out_shape=jax.ShapeDtypeStruct((rows, cols), F32),
        cost_estimate=cost(2, rows, cols), name="cut", compiler_params=PARAMS,
    )(at, x)


def calc_kernel(parcels, at, factor, m_ref, g_ref, *o_refs):
    for (start, rows), o_ref in zip(parcels, o_refs):
        part = pl.ds(start, rows)
        o_ref[...] = F32(0.9) * m_ref[part, :] + factor[0] * g_ref[part, :]


def calc(m, g, factor, at, cols, parcels):
    rows = m.shape[0]
    spec = pl.BlockSpec((rows, cols), lambda i, at: (0, at[0]))
    return pl.pallas_call(
        functools.partial(calc_kernel, parcels),
        grid_spec=pltpu.PrefetchScalarGridSpec(
            num_scalar_prefetch=1, grid=(1,),
            in_specs=[pl.BlockSpec(memory_space=pltpu.SMEM), spec, spec],
            out_specs=[pl.BlockSpec((r, cols), lambda i, at: (0, 0)) for _, r in parcels]),
        out_shape=[jax.ShapeDtypeStruct((r, cols), F32) for _, r in parcels],
        cost_estimate=cost(3, rows, cols), name="calc", compiler_params=PARAMS,
    )(at, factor, m, g)


def finish_kernel(parts, at, *refs):
    nw_ref, nm_ref = refs[-2:]
    for q in range(parts):
        @pl.when(pl.program_id(0) == q)
        def _():
            m = refs[2 * q + 1][...]
            nm_ref[...] = m
            nw_ref[...] = refs[2 * q][...] - F32(0.1) * m


def finish(at, pairs, outs, shape, piece, start, rows, within):
    cols = shape[1]
    b = block_rows(rows, start)
    s, p, o = start // b, piece // b, within // b
    parts = len(pairs)
    last = rows // b - 1

    def spec(part, first):
        def index(q, i, at):
            turn = jnp.where(q == part, i, jnp.where(q < part, 0, last))
            return (first + turn, 0)

        return pl.BlockSpec((b, cols), index if parts > 1 else lambda q, i, at: (first + i, 0))

    ospec = pl.BlockSpec((b, cols), lambda q, i, at: (at[q] * p + s + i, 0))
    hbm = pl.BlockSpec(memory_space=pl.ANY)
    return pl.pallas_call(
        functools.partial(finish_kernel, parts),
        grid_spec=pltpu.PrefetchScalarGridSpec(
            num_scalar_prefetch=1, grid=(parts, rows // b),
            in_specs=[spec(part, first) for part in range(parts) for first in (o, 0)] + [hbm] * 2, out_specs=[ospec, ospec]),
        out_shape=[jax.ShapeDtypeStruct(shape, F32)] * 2,
        input_output_aliases={2 * parts + 1: 0, 2 * parts + 2: 1},
        cost_estimate=cost(4 * parts, rows, cols), name="finish", compiler_params=PARAMS,
    )(at, *[x for pair in pairs for x in pair], *outs)


def own_kernel(at, factor, w_ref, m_ref, g_ref, nw_ref, nm_ref):
    m = F32(0.9) * m_ref[...] + factor[0] * g_ref[...]
    nm_ref[...] = m
    nw_ref[...] = w_ref[...] - F32(0.1) * m


def own(at, factor, w, m, g, n):
    rows, cols = w.shape[0], w.shape[1] // n
    b = block_rows(rows, 0)
    t = rows // b
    spec = pl.BlockSpec((b, cols), lambda i, at: (i, at[0]))
    ospec = pl.BlockSpec((b, cols), lambda i, at: (at[0] * t + i, 0))
    return pl.pallas_call(
        own_kernel,
        grid_spec=pltpu.PrefetchScalarGridSpec(
            num_scalar_prefetch=1, grid=(t,),
            in_specs=[pl.BlockSpec(memory_space=pltpu.SMEM)] + [spec] * 3, out_specs=[ospec, ospec]),
        out_shape=[jax.ShapeDtypeStruct((rows * n, cols), F32)] * 2,
        cost_estimate=cost(5, rows, cols), name="own", compiler_params=PARAMS,
    )(at, factor, w, m, g)


def squares_kernel(g_ref, o_ref, acc_ref):
    i = pl.program_id(0)
    rows, ff = g_ref.shape

    @pl.when(i == 0)
    def _():
        acc_ref[...] = jnp.zeros_like(acc_ref)

    for c in range(0, ff, LANES):
        g = g_ref[:, c:c + LANES]
        acc_ref[:, c:c + LANES] += jnp.sum((g * g).reshape(rows // 8, 8, LANES), axis=0)

    @pl.when(i == pl.num_programs(0) - 1)
    def _():
        parts = [acc_ref[:, c:c + LANES] for c in range(0, ff, LANES)]
        while len(parts) > 1:
            parts = [sum(parts[j:j + 2]) for j in range(0, len(parts), 2)]
        o_ref[...] = parts[0]


def squares(g):
    rows, ff = g.shape
    b = block_rows(rows, 0, 32)
    return pl.pallas_call(
        squares_kernel,
        grid=(rows // b,),
        in_specs=[pl.BlockSpec((b, ff), lambda i: (i, 0))],
        out_specs=pl.BlockSpec((8, LANES), lambda i: (0, 0)),
        out_shape=jax.ShapeDtypeStruct((8, LANES), F32),
        scratch_shapes=[pltpu.VMEM((8, ff), F32)],
        cost_estimate=cost(1, rows, ff), name="squares", compiler_params=PARAMS,
    )(g)


def last_pair(n):
    return [k for k in (4, 2) if k < n]


def w_parcels(k, n, rows):
    e = rows // 8
    if e % 8 == 0 and k == n - 1:
        return [(0, 2 * e), (2 * e, 2 * e), (4 * e, 4 * e)]
    return [(0, rows)]


SPLIT = lambda e: [(0, 4 * e), (4 * e, 2 * e), (6 * e, e), (7 * e, e)]


def m_parcels(k, n, rows):
    e = rows // 8
    if e % 8 == 0 and k in last_pair(n):
        return SPLIT(e)
    return w_parcels(k, n, rows)


def plan(n):
    far = list(range(n - 1, 3, -1))
    near = [k for k in (3, 2, 1) if k < n]
    return far, near


def body(limit, n, nrow, grad, momentum, weight):
    me = lax.axis_index("col")
    rows, ff = weight.shape
    cols = ff // n
    far, near = plan(n)
    at = {k: jnp.reshape(me ^ k, (1,)).astype(jnp.int32) for k in range(n)}
    moved_w, moved_m = {}, {}

    def send_w(k):
        for j, (s, r) in enumerate(w_parcels(k, n, rows)):
            moved_w[k, j] = hop(cut(weight, at[k], cols, s, r), "col", k, n)

    for k in far + near:
        send_w(k)
    part = squares(grad)
    bits = rounds(n, nrow)
    for axis, k, size in bits:
        part = part + hop(part, axis, k, size)
    total = jnp.sum(part)
    factor = jnp.reshape(jnp.minimum(F32(1.0), limit / (jnp.sqrt(total) + F32(1e-06))), (1,))
    for k in far + near:
        parts = calc(momentum, grad, factor, at[k], cols, m_parcels(k, n, rows))
        for j, part in enumerate(parts):
            moved_m[k, j] = hop(part, "col", k, n)
    outs = own(at[0], factor, weight, momentum, grad, n)
    for group in finish_order(n, rows):
        (s, r) = m_parcels(group[0][0], n, rows)[group[0][1]]
        pairs, where = [], []
        for k, j in group:
            i = max(i for i, (ws, _) in enumerate(w_parcels(k, n, rows)) if ws <= s)
            pairs.append((moved_w[k, i], moved_m[k, j]))
            where.append(at[k])
        within = s - w_parcels(group[0][0], n, rows)[i][0]
        outs = finish(jnp.concatenate(where), pairs, outs, (rows * n, cols), rows, s, r, within)
    return tuple(outs)


def finish_order(n, rows):
    end = last_pair(n)
    order = [1] + [k for k in range(n - 1, 1, -1) if k not in end]
    groups = [[(k, j)] for k in order for j in range(len(m_parcels(k, n, rows)))]
    for j in range(len(m_parcels(end[0], n, rows))):
        groups.append([(k, j) for k in end])
    return groups


def rounds(n, nrow):
    col = [("col", 1 << j, n) for j in range(n.bit_length() - 1)]
    row = [("row", 1 << j, nrow) for j in range(nrow.bit_length() - 1)]
    return col[2:] + col[:1] + row + col[1:2]


def solution(mesh):
    spec = P(("row", "col"), None)
    n, nrow = mesh.shape["col"], mesh.shape["row"]

    def run(grad, momentum, weight):
        limit = F32(math.sqrt(grad.shape[0] * grad.shape[1]))
        f = jax.shard_map(lambda g, m, w: body(limit, n, nrow, g, m, w), mesh=mesh, in_specs=(spec,) * 3, out_specs=(P("row", "col"),) * 2, check_vma=False)
        return f(grad, momentum, weight)

    return run
```

```python
import functools
import math

import jax
import jax.numpy as jnp
from jax import lax
from jax.experimental import pallas as pl
from jax.experimental.pallas import tpu as pltpu
from jax.sharding import PartitionSpec as P


F32 = jnp.float32
LANES = 128


def hop(x, axis, k, n):
    return lax.ppermute(x, axis, [(i, i ^ k) for i in range(n)])


def cost(passes, rows, cols):
    return pl.CostEstimate(flops=4 * rows * cols, bytes_accessed=4 * passes * rows * cols, transcendentals=0)


PARAMS = pltpu.CompilerParams(vmem_limit_bytes=67043328)


def block_rows(rows, start, most=256):
    b = most
    while rows % b or start % b:
        b //= 2
    return b


def copy_kernel(at, x_ref, o_ref):
    o_ref[...] = x_ref[...]


def cut(x, at, cols, start, rows):
    b = block_rows(rows, start)
    s = start // b
    return pl.pallas_call(
        copy_kernel,
        grid_spec=pltpu.PrefetchScalarGridSpec(
            num_scalar_prefetch=1, grid=(rows // b,),
            in_specs=[pl.BlockSpec((b, cols), lambda i, at: (s + i, at[0]))],
            out_specs=pl.BlockSpec((b, cols), lambda i, at: (i, 0))),
        out_shape=jax.ShapeDtypeStruct((rows, cols), F32),
        cost_estimate=cost(2, rows, cols), name="cut", compiler_params=PARAMS,
    )(at, x)


def calc_kernel(parcels, at, factor, m_ref, g_ref, *o_refs):
    for (start, rows), o_ref in zip(parcels, o_refs):
        part = pl.ds(start, rows)
        o_ref[...] = F32(0.9) * m_ref[part, :] + factor[0] * g_ref[part, :]


def calc(m, g, factor, at, cols, parcels):
    rows = m.shape[0]
    spec = pl.BlockSpec((rows, cols), lambda i, at: (0, at[0]))
    return pl.pallas_call(
        functools.partial(calc_kernel, parcels),
        grid_spec=pltpu.PrefetchScalarGridSpec(
            num_scalar_prefetch=1, grid=(1,),
            in_specs=[pl.BlockSpec(memory_space=pltpu.SMEM), spec, spec],
            out_specs=[pl.BlockSpec((r, cols), lambda i, at: (0, 0)) for _, r in parcels]),
        out_shape=[jax.ShapeDtypeStruct((r, cols), F32) for _, r in parcels],
        cost_estimate=cost(3, rows, cols), name="calc", compiler_params=PARAMS,
    )(at, factor, m, g)


def finish_kernel(parts, at, *refs):
    nw_ref, nm_ref = refs[-2:]
    for q in range(parts):
        @pl.when(pl.program_id(0) == q)
        def _():
            m = refs[2 * q + 1][...]
            nm_ref[...] = m
            nw_ref[...] = refs[2 * q][...] - F32(0.1) * m


def finish(at, pairs, outs, shape, piece, start, rows, within):
    cols = shape[1]
    b = block_rows(rows, start)
    s, p, o = start // b, piece // b, within // b
    parts = len(pairs)
    last = rows // b - 1

    def spec(part, first):
        def index(q, i, at):
            turn = jnp.where(q == part, i, jnp.where(q < part, 0, last))
            return (first + turn, 0)

        return pl.BlockSpec((b, cols), index if parts > 1 else lambda q, i, at: (first + i, 0))

    ospec = pl.BlockSpec((b, cols), lambda q, i, at: (at[q] * p + s + i, 0))
    hbm = pl.BlockSpec(memory_space=pl.ANY)
    return pl.pallas_call(
        functools.partial(finish_kernel, parts),
        grid_spec=pltpu.PrefetchScalarGridSpec(
            num_scalar_prefetch=1, grid=(parts, rows // b),
            in_specs=[spec(part, first) for part in range(parts) for first in (o, 0)] + [hbm] * 2, out_specs=[ospec, ospec]),
        out_shape=[jax.ShapeDtypeStruct(shape, F32)] * 2,
        input_output_aliases={2 * parts + 1: 0, 2 * parts + 2: 1},
        cost_estimate=cost(4 * parts, rows, cols), name="finish", compiler_params=PARAMS,
    )(at, *[x for pair in pairs for x in pair], *outs)


def last_finish_kernel(parts, s, p, rows, chunk, at, *refs):
    ins, (nw_hbm, nm_hbm), scratch = refs[:2 * parts], refs[2 * parts + 2:2 * parts + 4], refs[2 * parts + 4:]
    bufs, news, in_sem, out_sem = scratch[:2 * parts], scratch[2 * parts:3 * parts], scratch[-2], scratch[-1]
    chunks = [(q, r) for r in range(0, rows, chunk) for q in range(parts)]

    def load(q, j, r):
        ref = ins[2 * q + j]
        here = pl.ds(r, chunk)
        return pltpu.make_async_copy(ref.at[pl.ds(ref.shape[0] - rows + r, chunk)], bufs[2 * q + j].at[here], in_sem.at[2 * q + j, r // chunk])

    loads = {(q, j, r): load(q, j, r) for q, r in chunks for j in (1, 0)}
    for copy in loads.values():
        copy.start()
    stores = []
    for q, r in chunks:
        out = pl.ds(pl.multiple_of((at[q] * p + s) * rows + r, 8), chunk)
        here = pl.ds(r, chunk)
        loads[q, 1, r].wait()
        stores.append(pltpu.make_async_copy(bufs[2 * q + 1].at[here], nm_hbm.at[out], out_sem.at[2 * q + 1, r // chunk]))
        stores[-1].start()
        loads[q, 0, r].wait()
        news[q][here] = bufs[2 * q][here] - F32(0.1) * bufs[2 * q + 1][here]
        stores.append(pltpu.make_async_copy(news[q].at[here], nw_hbm.at[out], out_sem.at[2 * q, r // chunk]))
        stores[-1].start()
    for copy in stores:
        copy.wait()


def last_finish(at, pairs, outs, shape, piece, start, rows):
    cols = shape[1]
    parts = len(pairs)
    hbm = pl.BlockSpec(memory_space=pl.ANY)
    return pl.pallas_call(
        functools.partial(last_finish_kernel, parts, start // rows, piece // rows, rows, rows),
        in_specs=[pl.BlockSpec(memory_space=pltpu.SMEM)] + [hbm] * (2 * parts + 2), out_specs=[hbm, hbm],
        out_shape=[jax.ShapeDtypeStruct(shape, F32)] * 2,
        input_output_aliases={2 * parts + 1: 0, 2 * parts + 2: 1},
        scratch_shapes=[pltpu.VMEM((rows, cols), F32)] * (3 * parts) + [pltpu.SemaphoreType.DMA((2 * parts, 1))] * 2,
        cost_estimate=cost(4 * parts, rows, cols), name="last_finish", compiler_params=PARAMS,
    )(at, *[x for pair in pairs for x in pair], *outs)


def own_kernel(at, factor, w_ref, m_ref, g_ref, nw_ref, nm_ref):
    m = F32(0.9) * m_ref[...] + factor[0] * g_ref[...]
    nm_ref[...] = m
    nw_ref[...] = w_ref[...] - F32(0.1) * m


def own(at, factor, w, m, g, n):
    rows, cols = w.shape[0], w.shape[1] // n
    b = block_rows(rows, 0)
    t = rows // b
    spec = pl.BlockSpec((b, cols), lambda i, at: (i, at[0]))
    ospec = pl.BlockSpec((b, cols), lambda i, at: (at[0] * t + i, 0))
    return pl.pallas_call(
        own_kernel,
        grid_spec=pltpu.PrefetchScalarGridSpec(
            num_scalar_prefetch=1, grid=(t,),
            in_specs=[pl.BlockSpec(memory_space=pltpu.SMEM)] + [spec] * 3, out_specs=[ospec, ospec]),
        out_shape=[jax.ShapeDtypeStruct((rows * n, cols), F32)] * 2,
        cost_estimate=cost(5, rows, cols), name="own", compiler_params=PARAMS,
    )(at, factor, w, m, g)


def squares_kernel(g_ref, o_ref, acc_ref):
    i = pl.program_id(0)
    rows, ff = g_ref.shape

    @pl.when(i == 0)
    def _():
        acc_ref[...] = jnp.zeros_like(acc_ref)

    for c in range(0, ff, LANES):
        g = g_ref[:, c:c + LANES]
        acc_ref[:, c:c + LANES] += jnp.sum((g * g).reshape(rows // 8, 8, LANES), axis=0)

    @pl.when(i == pl.num_programs(0) - 1)
    def _():
        parts = [acc_ref[:, c:c + LANES] for c in range(0, ff, LANES)]
        while len(parts) > 1:
            parts = [sum(parts[j:j + 2]) for j in range(0, len(parts), 2)]
        o_ref[...] = parts[0]


def squares(g):
    rows, ff = g.shape
    b = block_rows(rows, 0, 32)
    return pl.pallas_call(
        squares_kernel,
        grid=(rows // b,),
        in_specs=[pl.BlockSpec((b, ff), lambda i: (i, 0))],
        out_specs=pl.BlockSpec((8, LANES), lambda i: (0, 0)),
        out_shape=jax.ShapeDtypeStruct((8, LANES), F32),
        scratch_shapes=[pltpu.VMEM((8, ff), F32)],
        cost_estimate=cost(1, rows, ff), name="squares", compiler_params=PARAMS,
    )(g)


def last_pair(n):
    return [k for k in (2, 4) if k < n]


def w_parcels(k, n, rows):
    e = rows // 8
    if e % 8 == 0 and k == n - 1:
        return [(0, 2 * e), (2 * e, 2 * e), (4 * e, 4 * e)]
    return [(0, rows)]


SPLIT = lambda e: [(0, 4 * e), (4 * e, 2 * e), (6 * e, e), (7 * e, e)]


def m_parcels(k, n, rows):
    e = rows // 8
    if e % 8 == 0 and k in last_pair(n):
        return SPLIT(e)
    return w_parcels(k, n, rows)


def plan(n):
    far = list(range(n - 1, 3, -1))
    near = [k for k in (3, 2, 1) if k < n]
    return far, near


def body(limit, n, nrow, grad, momentum, weight):
    me = lax.axis_index("col")
    rows, ff = weight.shape
    cols = ff // n
    far, near = plan(n)
    at = {k: jnp.reshape(me ^ k, (1,)).astype(jnp.int32) for k in range(n)}
    moved_w, moved_m = {}, {}

    def send_w(k):
        for j, (s, r) in enumerate(w_parcels(k, n, rows)):
            moved_w[k, j] = hop(cut(weight, at[k], cols, s, r), "col", k, n)

    for k in far + near:
        send_w(k)
    part = squares(grad)
    bits = rounds(n, nrow)
    for axis, k, size in bits:
        part = part + hop(part, axis, k, size)
    total = jnp.sum(part)
    factor = jnp.reshape(jnp.minimum(F32(1.0), limit / (jnp.sqrt(total) + F32(1e-06))), (1,))
    for k in far + near:
        parts = calc(momentum, grad, factor, at[k], cols, m_parcels(k, n, rows))
        for j, part in enumerate(parts):
            moved_m[k, j] = hop(part, "col", k, n)
    outs = own(at[0], factor, weight, momentum, grad, n)
    for group in finish_order(n, rows):
        (s, r) = m_parcels(group[0][0], n, rows)[group[0][1]]
        pairs, where = [], []
        for k, j in group:
            i = max(i for i, (ws, _) in enumerate(w_parcels(k, n, rows)) if ws <= s)
            pairs.append((moved_w[k, i], moved_m[k, j]))
            where.append(at[k])
        within = s - w_parcels(group[0][0], n, rows)[i][0]
        if s + r == rows and s and len(group) > 1:
            outs = last_finish(jnp.concatenate(where), pairs, outs, (rows * n, cols), rows, s, r)
        else:
            outs = finish(jnp.concatenate(where), pairs, outs, (rows * n, cols), rows, s, r, within)
    return tuple(outs)


def finish_order(n, rows):
    end = last_pair(n)
    order = [1] + [k for k in range(n - 1, 1, -1) if k not in end]
    groups = [[(k, j)] for k in order for j in range(len(m_parcels(k, n, rows)))]
    for j in range(len(m_parcels(end[0], n, rows))):
        groups.append([(k, j) for k in end])
    return groups


def rounds(n, nrow):
    col = [("col", 1 << j, n) for j in range(n.bit_length() - 1)]
    row = [("row", 1 << j, nrow) for j in range(nrow.bit_length() - 1)]
    return col[2:] + col[:1] + row + col[1:2]


def solution(mesh):
    spec = P(("row", "col"), None)
    n, nrow = mesh.shape["col"], mesh.shape["row"]

    def run(grad, momentum, weight):
        limit = F32(math.sqrt(grad.shape[0] * grad.shape[1]))
        f = jax.shard_map(lambda g, m, w: body(limit, n, nrow, g, m, w), mesh=mesh, in_specs=(spec,) * 3, out_specs=(P("row", "col"),) * 2, check_vma=False)
        return f(grad, momentum, weight)

    return run
```
